256 devices in a mesh: dp: 32 (over x, z), seq: 8 (over y, core).
Axes of the slice: x: 4, y: 4, z: 8, core: 2. Of those that a mesh axis runs over, the one named last changes fastest.
Arguments:
- hidden: bfloat16 [32, 8192, 4096], P('dp', 'seq'), may hold values from -6 to 6
- value_weight: bfloat16 [4096, 64], replicated, may hold values from -0.09375 to 0.09375
- value_bias: float32 [64], replicated, may hold values from -1 to 1
- returns: float32 [32, 8192], P('dp', 'seq'), may hold values from -12 to 12, as said below
- task_bins: int32 [32, 8192], P('dp', 'seq'), may hold values from 0 to 63
- loss_mask: int32 [32, 8192], P('dp', 'seq'), may hold values 0 or 1
Outputs:
- targets: float32 [32, 8192], P('dp', 'seq')
- weight_grad: float32 [4096, 64], replicated
- bias_grad: float32 [64], replicated
The draws below stay inside these ranges and needn't reach their ends.
Inputs may be any that keep to these rules, and one draw needn't show every extreme that they name: The returns of one rollout share a level and a trend along positions.
All inputs are finite; a program needn't handle non-finite values.
Results may differ from the reference program's by a relative error of at most 0.00083.
Values sent between devices are 32-bit elements.
A program may use at most 64 MiB of HBM per device.

```python
import math
import jax
import jax.numpy as jnp
import numpy as np
from jax import lax

D = 4096
NB = 64
ROLLOUTS = 32
LENGTH = 8192


def draw_returns(key, part):
    keys = jax.random.split(key, 4)
    level = jax.random.uniform(keys[0], (ROLLOUTS, 1), jnp.float32, -3.0, 3.0)
    noise = jnp.clip(jax.random.normal(keys[2], (ROLLOUTS, LENGTH), jnp.float32), -3.0, 3.0)
    trend = jax.random.uniform(keys[1], (ROLLOUTS, 1), jnp.float32, -2.0, 2.0)
    spread = jnp.exp(jax.random.uniform(keys[3], (ROLLOUTS, 1), jnp.float32, math.log(0.5), math.log(2.0)))
    position = jnp.arange(LENGTH, dtype=jnp.float32) / LENGTH
    return level + trend * position[None, :] + noise * spread


def plant(result, key, smallest, largest):
    extent = result.shape
    spot = [jax.random.randint(jax.random.fold_in(key, axis), (), 0, extent[axis]) for axis in range(len(extent))]
    result = result.at[tuple(spot)].set(smallest)
    longest = extent.index(max(extent))
    spot[longest] = (spot[longest] + 1) % extent[longest]
    return result.at[tuple(spot)].set(largest)


def steps_of(own_key, extent, shards, low, largest):
    factor_of, own = 1.0, jax.random.fold_in(own_key, 6)
    for axis_at, shards_of in shards:
        heights = jnp.exp(jax.random.uniform(jax.random.fold_in(own, axis_at), (shards_of,), jnp.float32, low / len(shards), largest / len(shards)))
        factor_of = factor_of * jnp.repeat(heights, extent[axis_at] // shards_of).reshape([-1 if axis == axis_at else 1 for axis in range(len(extent))])
    return factor_of


def cumulative_ranks(number_of, skew):
    weights = [(1 << 20) // math.isqrt(grade ** skew) + 1 for grade in range(1, number_of + 1)]
    scale = 1 + sum(weights) // (1 << 30)
    return np.cumsum(np.array([max(1, weight // scale) for weight in weights]))


def skewed_ids(key, shape, number_of, skew):
    grid = cumulative_ranks(number_of, skew)
    pick = jax.random.randint(jax.random.fold_in(key, 1), shape, 0, int(grid[number_of - 1]))
    grade = jnp.searchsorted(jnp.asarray(grid, jnp.int32), pick, side="right")
    return jax.random.permutation(jax.random.fold_in(key, 2), number_of)[grade].astype(jnp.int32)


def centred(own_key, extent, scale, most, shards=(), kind=jnp.bfloat16):
    drawn = scale * jax.random.normal(own_key, extent, jnp.float32)
    if shards:
        drawn = drawn * steps_of(own_key, extent, shards, -0.22, 0.18)
    return jnp.clip(drawn, -most, most).astype(kind)


def setup_inputs(seed: int = 0) -> dict:
    arg_keys = jax.random.split(jax.random.key(seed), 7)
    hidden = centred(arg_keys[0], (ROLLOUTS, LENGTH, D), 1.0, 6.0, ((0, 32), (1, 8)))
    value_weight = centred(arg_keys[1], (D, NB), D ** -0.5, 0.09375)
    value_bias = jnp.clip(jax.random.uniform(arg_keys[2], (NB,), jnp.float32, -1.0, 1.0), -1.0, 1.0)
    returns = draw_returns(jax.random.fold_in(arg_keys[6], 71), 0)
    task_bins = plant(skewed_ids(arg_keys[4], (ROLLOUTS, LENGTH), NB, 2), jax.random.fold_in(arg_keys[4], 3), 0, NB - 1).astype(jnp.int32)
    loss_mask = plant((jax.random.randint(arg_keys[5], (ROLLOUTS, LENGTH), 0, 4) < 3).astype(jnp.int32), jax.random.fold_in(arg_keys[5], 1), 0, 1)
    return {"hidden": hidden, "value_weight": value_weight, "value_bias": value_bias, "returns": returns, "task_bins": task_bins, "loss_mask": loss_mask}


def reference(hidden, value_weight, value_bias, returns, task_bins, loss_mask):
    bins_iota = jnp.arange(NB, dtype=jnp.int32)
    chosen = (task_bins[..., None] == bins_iota).astype(jnp.float32)
    onehot = chosen * loss_mask[..., None].astype(jnp.float32)
    counts = lax.optimization_barrier(jnp.sum(onehot, axis=(0, 1)))
    floor_counts = jnp.maximum(counts, 1.0)
    means = lax.optimization_barrier(jnp.sum(onehot * returns[..., None], axis=(0, 1))) / floor_counts
    deviation = returns[..., None] - means
    second = lax.optimization_barrier(jnp.sum(onehot * deviation * deviation, axis=(0, 1)))
    spread = jnp.sqrt(second / floor_counts + 0.1)
    targets = lax.optimization_barrier(jnp.sum(chosen * (deviation / spread), axis=-1))

    def rollout_step(running, slices):
        states, target_row, chosen_row, valid = slices
        scores = jnp.dot(states, value_weight, preferred_element_type=jnp.float32)
        predicted = lax.optimization_barrier(jnp.sum((scores + value_bias) * chosen_row, axis=-1))
        slope = valid * jnp.clip(predicted - target_row, -1.0, 1.0) / ROLLOUTS
        coefficient = chosen_row * slope[:, None]
        weight_part = lax.dot_general(states, coefficient.astype(jnp.bfloat16), (((0,), (0,)), ((), ())), preferred_element_type=jnp.float32)
        return ((running[0] + weight_part, running[1] + lax.optimization_barrier(jnp.sum(coefficient, axis=0))), None)
    start = (jnp.zeros((D, NB), jnp.float32), jnp.zeros((NB,), jnp.float32))
    (weight_grad, bias_grad), unused = lax.scan(rollout_step, start, (hidden, targets, chosen, loss_mask.astype(jnp.float32)))
    return (targets, weight_grad, bias_grad)
```

```python
import functools

import jax
import jax.numpy as jnp
from jax import lax
from jax.experimental import pallas as pl
from jax.experimental.pallas import tpu as pltpu
from jax.sharding import Mesh
from jax.sharding import PartitionSpec as P

NX, NZ, NY, NC = 4, 8, 4, 2
MESH = pl.DeviceIdType.MESH
HIGHEST = lax.Precision.HIGHEST
TOKENS, D, NB = 1024, 4096, 64
PIECES = 4
ROWS = TOKENS // PIECES
BLOCK = 512
HALF = D // 2
LAG = 3
ORDER = ((0, 2), (1, 2), (0, 1), (1, 1), (0, 3), (1, 3), (0, 0), (1, 0))


def dot(a, b, dims, precision=None):
    return lax.dot_general(a, b, (dims, ((), ())), precision=precision, preferred_element_type=jnp.float32)


def kernel(
    rollouts,
    hidden_hbm, weight_hbm, bias_hbm, returns_hbm, bins_hbm, mask_hbm,
    targets_ref, grad_ref, bias_grad_ref,
    hidden, weight, bias, returns, bins, mask,
    predicted, coefficient,
    stats_line, stats_plane, bias_line, bias_plane,
    parts, from_core, summed, got_first, kept, got_second, tiles, got_third,
    hidden_sem, in_sem, small_send, small_recv,
    core_send, core_recv, first_send, first_recv, second_send, second_recv, third_send, third_recv,
    back_third_send, back_third_recv, back_second_send, back_second_recv,
    back_first_send, back_first_recv, back_core_send, back_core_recv,
):
    x, z, y, c = (lax.axis_index(name) for name in ("x", "z", "y", "c"))

    def at(x=x, z=z, y=y, c=c):
        return {"x": x, "z": z, "y": y, "c": c}

    loads = [
        pltpu.make_async_copy(src, dst, in_sem.at[i])
        for i, (src, dst) in enumerate(
            ((returns_hbm, returns), (bins_hbm, bins), (mask_hbm, mask), (bias_hbm, bias), (weight_hbm, weight))
        )
    ]
    for load in loads:
        load.start()
    pieces = [
        pltpu.make_async_copy(
            hidden_hbm.at[0, pl.ds(i * ROWS, ROWS)], hidden.at[pl.ds(i * ROWS, ROWS)], hidden_sem.at[i]
        )
        for i in range(PIECES)
    ]
    for piece in pieces:
        piece.start()

    barrier = pltpu.get_barrier_semaphore()

    def in_line(k):
        return at(z=lax.rem(z + k // 2, NZ), c=lax.rem(c + k, NC))

    def in_plane(k):
        return at(x=lax.rem(x + k // NY, NX), y=lax.rem(y + k, NY))

    def greet(k, carry):
        pl.semaphore_signal(barrier, inc=1, device_id=in_line(k), device_id_type=MESH)
        pl.semaphore_signal(barrier, inc=1, device_id=in_plane(k), device_id_type=MESH)
        return carry

    lax.fori_loop(1, 16, greet, 0)

    def send_all(buffer, slot, sem, peer):
        def body(k, carry):
            pltpu.make_async_remote_copy(
                src_ref=buffer.at[slot],
                dst_ref=buffer.at[slot],
                send_sem=small_send.at[sem],
                recv_sem=small_recv.at[sem],
                device_id=peer(k),
                device_id_type=MESH,
            ).start()
            return carry

        lax.fori_loop(1, 16, body, 0)

    def wait_all(buffer, sems, sem):
        fifteen = buffer.at[pl.ds(0, 15)]
        pltpu.make_async_copy(fifteen, fifteen, sems.at[sem]).wait()

    my_line = z * NC + c
    my_plane = x * NY + y

    for load in loads[:3]:
        load.wait()
    ret = returns[...]
    ids = bins[...]
    valid = mask[...].astype(jnp.float32)
    chosen = (lax.broadcasted_iota(jnp.int32, (NB, TOKENS), 0) == ids).astype(jnp.float32)
    row = lax.broadcasted_iota(jnp.int32, (8, TOKENS), 0)
    moments = jnp.where(row == 0, valid, jnp.where(row == 1, valid * ret, jnp.where(row == 2, valid * ret * ret, 0.0)))
    local = dot(moments, chosen, ((1,), (1,)), HIGHEST)
    padding = jnp.zeros((8, 128 - NB), jnp.float32)
    stats_line[my_line] = jnp.concatenate([local, padding], axis=1)

    pl.semaphore_wait(barrier, 30)
    send_all(stats_line, my_line, 0, in_line)

    loads[4].wait()
    for i in range(PIECES):
        pieces[i].wait()
        scores = dot(weight[...], hidden[pl.ds(i * ROWS, ROWS), :], ((1,), (1,)))
        predicted[:, pl.ds(i * ROWS, ROWS)] = jnp.sum(
            jnp.where(lax.broadcasted_iota(jnp.int32, (NB, ROWS), 0) == bins[:, pl.ds(i * ROWS, ROWS)], scores, 0.0),
            axis=0,
            keepdims=True,
        )

    wait_all(stats_line, small_recv, 0)
    total = stats_line[0]
    for i in range(1, 16):
        total = total + stats_line[i]
    stats_plane[my_plane] = total
    send_all(stats_plane, my_plane, 1, in_plane)
    loads[3].wait()
    wait_all(stats_plane, small_recv, 1)
    total = stats_plane[0]
    for i in range(1, 16):
        total = total + stats_plane[i]

    counts = jnp.maximum(total[0:1, :NB], 1.0)
    means = total[1:2, :NB] / counts
    second = total[2:3, :NB] - total[1:2, :NB] * means
    spread = jnp.sqrt(second / counts + 0.1)
    table_row = lax.broadcasted_iota(jnp.int32, (8, NB), 0)
    table = jnp.where(
        table_row == 0, means, jnp.where(table_row == 1, spread, jnp.where(table_row == 2, bias[...], 0.0))
    )
    chosen = (lax.broadcasted_iota(jnp.int32, (NB, TOKENS), 0) == bins[...]).astype(jnp.float32)
    own = dot(table, chosen, ((1,), (0,)), HIGHEST)
    targets = (returns[...] - own[0:1]) / own[1:2]
    targets_ref[...] = targets
    slope = mask[...].astype(jnp.float32) * jnp.clip(predicted[...] + own[2:3] - targets, -1.0, 1.0) / rollouts
    coefficient[...] = (chosen * slope).astype(jnp.bfloat16)
    slopes = jnp.where(row == 0, slope, 0.0)
    local = dot(slopes, chosen, ((1,), (1,)), HIGHEST)
    bias_line[my_line] = jnp.concatenate([local, padding], axis=1)
    send_all(bias_line, my_line, 2, in_line)

    mine = pl.ds(pl.multiple_of(c * 32, 32), 32)
    others = pl.ds(pl.multiple_of((1 - c) * 32, 32), 32)
    sizes = (NX, NY)

    def first_peer(half, k):
        return at(x=lax.rem(x + k, NX)) if half == 0 else at(y=lax.rem(y + k, NY))

    def second_peer(half, k):
        return at(y=lax.rem(y + k, NY)) if half == 0 else at(x=lax.rem(x + k, NX))

    first_at, second_at = (x, y), (y, x)

    def copy(src, dst, send, recv, peer):
        return pltpu.make_async_remote_copy(
            src_ref=src, dst_ref=dst, send_sem=send, recv_sem=recv, device_id=peer, device_id_type=MESH
        )

    sent = []

    def core_copy(s):
        return copy(parts.at[s, others], from_core.at[s], core_send.at[s], core_recv.at[s], at(c=1 - c))

    def first_copy(s):
        half, k = ORDER[s]
        return copy(
            summed.at[s], got_first.at[half, k - 1], first_send.at[half, k - 1], first_recv.at[half, k - 1],
            first_peer(half, k),
        )

    def finish(s):
        core_copy(s).wait_recv()
        summed[s] = parts[s, mine] + from_core[s]
        if ORDER[s][1]:
            first_copy(s).start()

    for s, (half, k) in enumerate(ORDER):
        owner = lax.rem(first_at[half] + k, 4)
        columns = pl.ds(pl.multiple_of(half * HALF + owner * BLOCK, BLOCK), BLOCK)
        parts[s] = dot(coefficient[...], hidden[:, columns], ((1,), (0,)))
        core_copy(s).start()
        if s >= LAG:
            finish(s - LAG)
    for s in range(len(ORDER) - LAG, len(ORDER)):
        finish(s)

    wait_all(bias_line, small_recv, 2)
    total = bias_line[0]
    for i in range(1, 16):
        total = total + bias_line[i]
    bias_plane[my_plane] = total
    send_all(bias_plane, my_plane, 3, in_plane)

    def second_copy(half, k):
        there = lax.rem(second_at[half] + k, 4)
        return copy(
            kept.at[half, :, pl.ds(pl.multiple_of(there * 128, 128), 128)], got_second.at[half, k - 1],
            second_send.at[half, k - 1], second_recv.at[half, k - 1], second_peer(half, k),
        )

    for half in range(2):
        s = ORDER.index((half, 0))
        for k in (1, 3, 2):
            first_copy(ORDER.index((half, k))).wait_recv()
        kept[half] = summed[s] + got_first[half, 0] + got_first[half, 1] + got_first[half, 2]
        for k in (2, 1, 3):
            second_copy(half, k).start()

    def third_copy(k):
        there = lax.rem(z + k, NZ)
        return copy(tiles.at[there], got_third.at[k - 1], third_send.at[k - 1], third_recv.at[k - 1], at(z=there))

    for half in range(2):
        for k in (1, 3, 2):
            second_copy(half, k).wait_recv()
        here = pl.ds(pl.multiple_of(second_at[half] * 128, 128), 128)
        block = kept[half, :, here] + got_second[half, 0] + got_second[half, 1] + got_second[half, 2]
        for i in range(4):
            tiles[half * 4 + i] = block[i * 8 : i * 8 + 8]
    for k in (4, 3, 5, 2, 6, 1, 7):
        third_copy(k).start()
    for k in (1, 7, 2, 6, 3, 5, 4):
        third_copy(k).wait_recv()
    tile = tiles[z]
    for k in range(1, NZ):
        tile = tile + got_third[k - 1]

    column_of = (x * BLOCK + y * 128, HALF + y * BLOCK + x * 128)
    high = z // 4
    place = grad_ref.at[
        pl.ds(pl.multiple_of(c * 32 + (z - 4 * high) * 8, 8), 8),
        pl.ds(pl.multiple_of(column_of[0] + high * (column_of[1] - column_of[0]), 128), 128),
    ]
    place[...] = tile

    def back_third(k):
        return copy(place, place, back_third_send.at[k - 1], back_third_recv.at[k - 1], at(z=lax.rem(z + k, NZ)))

    def back_second(half, k):
        spot = grad_ref.at[mine, pl.ds(pl.multiple_of(column_of[half], 128), 128)]
        return copy(
            spot, spot, back_second_send.at[half, k - 1], back_second_recv.at[half, k - 1], second_peer(half, k)
        )

    def back_first(half, k):
        spot = grad_ref.at[mine, pl.ds(pl.multiple_of(half * HALF + first_at[half] * BLOCK, BLOCK), BLOCK)]
        return copy(spot, spot, back_first_send.at[half, k - 1], back_first_recv.at[half, k - 1], first_peer(half, k))

    def back_core(half, k):
        owner = lax.rem(first_at[half] + 4 - k, 4)
        spot = grad_ref.at[mine, pl.ds(pl.multiple_of(half * HALF + owner * BLOCK, BLOCK), BLOCK)]
        return copy(spot, spot, back_core_send.at[half, k], back_core_recv.at[half, k], at(c=1 - c))

    for k in (4, 3, 5, 2, 6, 1, 7):
        back_third(k).start()
    for k in (1, 7, 2, 6, 3, 5, 4):
        back_third(k).wait_recv()
    for half in range(2):
        for k in (2, 1, 3):
            back_second(half, k).start()
    for half in range(2):
        for k in (1, 3, 2):
            back_second(half, k).wait_recv()
        for k in (2, 1, 3):
            back_first(half, k).start()
        back_core(half, 0).start()

    wait_all(bias_plane, small_recv, 3)
    total = bias_plane[0]
    for i in range(1, 16):
        total = total + bias_plane[i]
    bias_grad_ref[...] = total[0:1, :NB]

    for k in (1, 3, 2):
        for half in range(2):
            back_first(half, k).wait_recv()
            back_core(half, k).start()
    for half in range(2):
        for k in range(4):
            back_core(half, k).wait_recv()

    for i, buffer in enumerate((stats_line, stats_plane, bias_line, bias_plane)):
        wait_all(buffer, small_send, i)
    for s, (half, k) in enumerate(ORDER):
        core_copy(s).wait_send()
        if k:
            first_copy(s).wait_send()
            second_copy(half, k).wait_send()
            back_second(half, k).wait_send()
            back_first(half, k).wait_send()
        back_core(half, k).wait_send()
    for k in range(1, NZ):
        third_copy(k).wait_send()
        back_third(k).wait_send()


def on_device(hidden, value_weight, value_bias, returns, task_bins, loss_mask):
    rollouts = hidden.shape[0] * lax.axis_size(("x", "z"))
    f32 = jnp.float32
    dma = pltpu.SemaphoreType.DMA
    any_space = pl.BlockSpec(memory_space=pl.ANY)
    vmem = pl.BlockSpec(memory_space=pltpu.VMEM)
    small = pltpu.VMEM((16, 8, 128), f32)
    targets, grad, bias_grad = pl.pallas_call(
        functools.partial(kernel, rollouts),
        out_shape=(
            jax.ShapeDtypeStruct((1, TOKENS), f32),
            jax.ShapeDtypeStruct((NB, D), f32),
            jax.ShapeDtypeStruct((1, NB), f32),
        ),
        in_specs=[any_space] * 6,
        out_specs=(vmem, vmem, vmem),
        scratch_shapes=[
            pltpu.VMEM((TOKENS, D), jnp.bfloat16),
            pltpu.VMEM((NB, D), jnp.bfloat16),
            pltpu.VMEM((1, NB), f32),
            pltpu.VMEM((1, TOKENS), f32),
            pltpu.VMEM((1, TOKENS), jnp.int32),
            pltpu.VMEM((1, TOKENS), jnp.int32),
            pltpu.VMEM((1, TOKENS), f32),
            pltpu.VMEM((NB, TOKENS), jnp.bfloat16),
            small, small, small, small,
            pltpu.VMEM((8, NB, BLOCK), f32),
            pltpu.VMEM((8, 32, BLOCK), f32),
            pltpu.VMEM((8, 32, BLOCK), f32),
            pltpu.VMEM((2, 3, 32, BLOCK), f32),
            pltpu.VMEM((2, 32, BLOCK), f32),
            pltpu.VMEM((2, 3, 32, 128), f32),
            pltpu.VMEM((8, 8, 128), f32),
            pltpu.VMEM((7, 8, 128), f32),
            dma((PIECES,)), dma((5,)), dma((4,)), dma((4,)),
            dma((8,)), dma((8,)), dma((2, 3)), dma((2, 3)), dma((2, 3)), dma((2, 3)), dma((7,)), dma((7,)),
            dma((7,)), dma((7,)), dma((2, 3)), dma((2, 3)), dma((2, 3)), dma((2, 3)), dma((2, 4)), dma((2, 4)),
        ],
        compiler_params=pltpu.CompilerParams(
            collective_id=0, has_side_effects=True, vmem_limit_bytes=60 * 1024 * 1024
        ),
    )(hidden, value_weight.T, value_bias.reshape(1, NB), returns, task_bins, loss_mask)
    return targets, grad.T, bias_grad.reshape(NB)


def solution(mesh):
    torus = Mesh(mesh.devices.reshape(NX, NZ, NY, NC), ("x", "z", "y", "c"))
    dp, seq = ("x", "z"), ("y", "c")
    return jax.shard_map(
        on_device,
        mesh=torus,
        in_specs=(P(dp, seq, None), P(), P(), P(dp, seq), P(dp, seq), P(dp, seq)),
        out_specs=(P(dp, seq), P(), P()),
        check_vma=False,
    )
```

```python
import functools

import jax
import jax.numpy as jnp
from jax import lax
from jax.experimental import pallas as pl
from jax.experimental.pallas import tpu as pltpu
from jax.sharding import Mesh
from jax.sharding import PartitionSpec as P

NX, NZ, NY, NC = 4, 8, 4, 2
MESH = pl.DeviceIdType.MESH
HIGHEST = lax.Precision.HIGHEST
TOKENS, D, NB = 1024, 4096, 64
PIECES = 2
ROWS = TOKENS // PIECES
BLOCK = 512
HALF = D // 2
QUARTER = 256
PAIRS = ((2, 1), (3, 0))


def ring(k, n):
    return min(k, n - k)


LINE = sorted(((k, c) for k in range(NZ) for c in range(NC) if k or c), key=lambda p: -ring(p[0], NZ))
PLANE = sorted(((i, j) for i in range(NX) for j in range(NY) if i or j), key=lambda p: -ring(p[0], NX) - ring(p[1], NY))


def dot(a, b, dims, precision=None):
    return lax.dot_general(a, b, (dims, ((), ())), precision=precision, preferred_element_type=jnp.float32)


def ordered_sum(parts):
    total = parts[0]
    for part in parts[1:]:
        total = total + part
    return total


def kernel(
    rollouts,
    hidden_hbm, weight_hbm, bias_hbm, returns_hbm, bins_hbm, mask_hbm,
    targets_ref, grad_ref, bias_grad_ref,
    hidden, weight, bias, returns, bins, mask,
    predicted, coefficient,
    stats_line, stats_plane, bias_line, bias_plane,
    parts, from_core, summed, got_first, kept, got_second, got_third,
    hidden_sem, in_sem, small_send, small_recv,
    core_send, core_recv, first_send, first_recv, second_send, second_recv, third_send, third_recv,
    back_second_send, back_second_recv, back_first_send, back_first_recv, back_core_send, back_core_recv,
):
    x, z, y, c = (lax.axis_index(name) for name in ("x", "z", "y", "c"))

    def at(x=x, z=z, y=y, c=c):
        return {"x": x, "z": z, "y": y, "c": c}

    def in_line(k, core):
        return at(z=lax.rem(z + k, NZ), c=lax.rem(c + core, NC))

    def in_plane(i, j):
        return at(x=lax.rem(x + i, NX), y=lax.rem(y + j, NY))

    loads = [
        pltpu.make_async_copy(src, dst, in_sem.at[i])
        for i, (src, dst) in enumerate(
            ((returns_hbm, returns), (bins_hbm, bins), (mask_hbm, mask), (bias_hbm, bias), (weight_hbm, weight))
        )
    ]
    pieces = [
        pltpu.make_async_copy(
            hidden_hbm.at[0, pl.ds(i * ROWS, ROWS)], hidden.at[pl.ds(i * ROWS, ROWS)], hidden_sem.at[i]
        )
        for i in range(PIECES)
    ]
    for load in loads[:3]:
        load.start()
    barrier = pltpu.get_barrier_semaphore()
    for near, far in zip(LINE, PLANE):
        pl.semaphore_signal(barrier, inc=1, device_id=in_line(*near), device_id_type=MESH)
        pl.semaphore_signal(barrier, inc=1, device_id=in_plane(*far), device_id_type=MESH)
    for load in (loads[4], *pieces, loads[3]):
        load.start()

    def copy(src, dst, send, recv, peer):
        return pltpu.make_async_remote_copy(
            src_ref=src, dst_ref=dst, send_sem=send, recv_sem=recv, device_id=peer, device_id_type=MESH
        )

    def send_all(buffer, slot, sem, peers):
        for peer in peers:
            copy(buffer.at[slot], buffer.at[slot], small_send.at[sem], small_recv.at[sem], peer).start()

    def wait_all(buffer, sems, sem):
        fifteen = buffer.at[pl.ds(0, 15)]
        pltpu.make_async_copy(fifteen, fifteen, sems.at[sem]).wait()

    def total_of(buffer):
        return ordered_sum([buffer[i] for i in range(16)])

    line_peers = [in_line(*p) for p in LINE]
    plane_peers = [in_plane(*p) for p in PLANE]
    my_line = z * NC + c
    my_plane = x * NY + y

    for load in loads[:3]:
        load.wait()
    ret = returns[...]
    valid = mask[...].astype(jnp.float32)
    twice = ((lax.broadcasted_iota(jnp.int32, (2 * NB, TOKENS), 0) & (NB - 1)) == bins[...]).astype(jnp.float32)
    row = lax.broadcasted_iota(jnp.int32, (8, TOKENS), 0)
    moments = jnp.where(row == 0, valid, jnp.where(row == 1, valid * ret, jnp.where(row == 2, valid * ret * ret, 0.0)))
    local = dot(moments, twice, ((1,), (1,)), HIGHEST)
    lane = lax.broadcasted_iota(jnp.int32, (1, 2 * NB), 1)
    stats_line[my_line, 0:1] = jnp.where(lane < NB, local[0:1], local[1:2])
    stats_line[my_line, 1:2] = local[2:3]

    pl.semaphore_wait(barrier, 30)
    send_all(stats_line, my_line, 0, line_peers)

    def score(i):
        pieces[i].wait()
        rows = pl.ds(i * ROWS, ROWS)
        scores = dot(weight[...], hidden[rows, :], ((1,), (1,)))
        match = lax.broadcasted_iota(jnp.int32, (NB, ROWS), 0) == bins[:, rows]
        predicted[:, rows] = jnp.sum(jnp.where(match, scores, 0.0), axis=0, keepdims=True)

    loads[4].wait()
    score(0)
    wait_all(stats_line, small_recv, 0)
    stats_plane[my_plane] = total_of(stats_line)
    send_all(stats_plane, my_plane, 1, plane_peers)
    score(1)
    loads[3].wait()
    wait_all(stats_line, small_send, 0)
    wait_all(stats_plane, small_recv, 1)
    total = total_of(stats_plane)

    counts = jnp.maximum(total[0:1, :NB], 1.0)
    sums = total[0:1, NB:]
    means = sums / counts
    second = total[1:2, :NB] - sums * means
    spread = jnp.sqrt(second / counts + 0.1)
    table_row = lax.broadcasted_iota(jnp.int32, (8, NB), 0)
    table = jnp.where(
        table_row == 0, means, jnp.where(table_row == 1, spread, jnp.where(table_row == 2, bias[...], 0.0))
    )
    chosen = (lax.broadcasted_iota(jnp.int32, (NB, TOKENS), 0) == bins[...]).astype(jnp.float32)
    own = dot(table, chosen, ((1,), (0,)), HIGHEST)
    targets = (returns[...] - own[0:1]) / own[1:2]
    targets_ref[...] = targets
    slope = mask[...].astype(jnp.float32) * jnp.clip(predicted[...] + own[2:3] - targets, -1.0, 1.0) / rollouts
    predicted[...] = slope
    coefficient[...] = (chosen * slope).astype(jnp.bfloat16)

    mine = pl.ds(pl.multiple_of(c * 32, 32), 32)
    others = pl.ds(pl.multiple_of((1 - c) * 32, 32), 32)
    first_at, second_at = (x, y), (y, x)

    def first_peer(half, k):
        return at(x=lax.rem(x + k, NX)) if half == 0 else at(y=lax.rem(y + k, NY))

    def second_peer(half, k):
        return at(y=lax.rem(y + k, NY)) if half == 0 else at(x=lax.rem(x + k, NX))

    def parity(group):
        return lax.rem(z + 1 + group, 2)

    def core_copy(s):
        return copy(parts.at[s, others], from_core.at[s], core_send.at[s], core_recv.at[s], at(c=1 - c))

    def first_copy(group, half, k):
        pair = next(i for i, ks in enumerate(PAIRS) if k in ks)
        spot = (PAIRS[pair].index(k) * 2 + half) * QUARTER
        return copy(
            summed.at[group * 2 + pair, :, pl.ds(spot, QUARTER)], got_first.at[group, half, k - 1],
            first_send.at[group, half, k - 1], first_recv.at[group, half, k - 1], first_peer(half, k),
        )

    for group in range(2):
        for pair, ks in enumerate(PAIRS):
            s = group * 2 + pair
            blocks = [
                hidden[:, pl.ds(
                    pl.multiple_of(
                        half * HALF + lax.rem(first_at[half] + k, 4) * BLOCK + parity(group) * QUARTER, QUARTER
                    ), QUARTER
                )]
                for k in ks for half in range(2)
            ]
            parts[s] = dot(coefficient[...], jnp.concatenate(blocks, axis=1), ((1,), (0,)))
            core_copy(s).start()
    for group in range(2):
        for pair, ks in enumerate(PAIRS):
            s = group * 2 + pair
            core_copy(s).wait_recv()
            summed[s] = parts[s, mine] + from_core[s]
            for k in ks:
                if k:
                    for half in range(2):
                        first_copy(group, half, k).start()

    chosen = (lax.broadcasted_iota(jnp.int32, (2 * NB, TOKENS), 0) == bins[...]).astype(jnp.float32)
    slopes = jnp.where(row == 0, predicted[...], 0.0)
    bias_line[my_line] = dot(slopes, chosen, ((1,), (1,)), HIGHEST)[0:1]
    send_all(bias_line, my_line, 2, line_peers)
    wait_all(stats_plane, small_send, 1)

    def second_copy(half, k):
        there = lax.rem(z + k, NZ)
        return copy(
            kept.at[(k + 1) % 2, half, pl.ds(pl.multiple_of(there // 2 * 8, 8), 8)], got_second.at[half, k - 1],
            second_send.at[half, k - 1], second_recv.at[half, k - 1], at(z=there),
        )

    for group, distances in enumerate(((3, 5, 1, 7), (4, 2, 6))):
        for half in range(2):
            for k in (1, 3, 2):
                first_copy(group, half, k).wait_recv()
            own_part = summed[group * 2 + 1, :, (2 + half) * QUARTER : (3 + half) * QUARTER]
            kept[group, half] = ordered_sum([own_part] + [got_first[group, half, i] for i in range(3)])
            for k in distances:
                second_copy(half, k).start()
    for s in range(4):
        core_copy(s).wait_send()

    wait_all(bias_line, small_recv, 2)
    bias_plane[my_plane] = total_of(bias_line)
    send_all(bias_plane, my_plane, 3, plane_peers)
    wait_all(bias_line, small_send, 2)

    def third_copy(half, k):
        slot = got_third.at[half, second_at[half]]
        return copy(slot, slot, third_send.at[half, k - 1], third_recv.at[half, k - 1], second_peer(half, k))

    for half in range(2):
        for k in (1, 7, 2, 6, 3, 5, 4):
            second_copy(half, k).wait_recv()
        own_part = kept[1, half, pl.ds(pl.multiple_of(z // 2 * 8, 8), 8)]
        got_third[half, second_at[half]] = ordered_sum([own_part] + [got_second[half, i] for i in range(7)])
        for k in (2, 1, 3):
            third_copy(half, k).start()
    for group in range(2):
        for half in range(2):
            for k in (1, 2, 3):
                first_copy(group, half, k).wait_send()

    def place(half, z):
        return grad_ref.at[
            pl.ds(pl.multiple_of(c * 32 + z // 2 * 8, 8), 8),
            pl.ds(pl.multiple_of(half * HALF + first_at[half] * BLOCK + lax.rem(z, 2) * QUARTER, QUARTER), QUARTER),
        ]

    def back_second(half, k):
        spot = place(half, z)
        return copy(
            spot, spot, back_second_send.at[half, k - 1], back_second_recv.at[half, k - 1], at(z=lax.rem(z + k, NZ))
        )

    def block_of(half, owner):
        return grad_ref.at[mine, pl.ds(pl.multiple_of(half * HALF + owner * BLOCK, BLOCK), BLOCK)]

    def back_first_part(half, k, distance):
        spot = place(half, lax.rem(z + NZ - distance, NZ))
        return copy(spot, spot, back_first_send.at[half, k - 1], back_first_recv.at[half, k - 1], first_peer(half, k))

    def back_first(half, k):
        spot = block_of(half, first_at[half])
        return copy(spot, spot, back_first_send.at[half, k - 1], back_first_recv.at[half, k - 1], first_peer(half, k))

    def back_core(half, k):
        spot = block_of(half, lax.rem(first_at[half] + 4 - k, 4))
        return copy(spot, spot, back_core_send.at[half, k], back_core_recv.at[half, k], at(c=1 - c))

    for half in range(2):
        for k in (1, 3, 2):
            third_copy(half, k).wait_recv()
        place(half, z)[...] = ordered_sum([got_third[half, i] for i in range(4)])
        for k in (4, 3, 5, 2, 6, 1, 7):
            back_second(half, k).start()
    for half in range(2):
        for k in range(1, NZ):
            second_copy(half, k).wait_send()
        for k in (1, 2, 3):
            third_copy(half, k).wait_send()
    for distance in (0, 1, 7, 2, 6, 3, 5, 4):
        for half in range(2):
            if distance:
                back_second(half, distance).wait_recv()
            for k in (2, 1, 3):
                back_first_part(half, k, distance).start()
    for half in range(2):
        back_core(half, 0).start()

    wait_all(bias_plane, small_recv, 3)
    bias_grad_ref[...] = total_of(bias_plane)[0:1, :NB]
    wait_all(bias_plane, small_send, 3)
    for half in range(2):
        for k in range(1, NZ):
            back_second(half, k).wait_send()

    for k in (1, 3, 2):
        for half in range(2):
            back_first(half, k).wait_recv()
            back_core(half, k).start()
    for half in range(2):
        for k in (1, 2, 3):
            back_first(half, k).wait_send()
    for k in (0, 1, 3, 2):
        for half in range(2):
            back_core(half, k).wait()


def write_out(targets, grad, bias_grad, targets_hbm, grad_hbm, bias_grad_hbm, sem):
    copies = [
        pltpu.make_async_copy(src, dst, sem.at[i])
        for i, (src, dst) in enumerate(
            ((grad, grad_hbm), (targets, targets_hbm), (bias_grad, bias_grad_hbm))
        )
    ]
    for copy in copies:
        copy.start()
    for copy in copies:
        copy.wait()


def on_device(hidden, value_weight, value_bias, returns, task_bins, loss_mask):
    rollouts = hidden.shape[0] * lax.axis_size(("x", "z"))
    f32 = jnp.float32
    dma = pltpu.SemaphoreType.DMA
    any_space = pl.BlockSpec(memory_space=pl.ANY)
    vmem = pl.BlockSpec(memory_space=pltpu.VMEM)
    pair, single = pltpu.VMEM((16, 2, 128), f32), pltpu.VMEM((16, 1, 128), f32)
    shapes = ((1, TOKENS), (NB, D), (1, NB))
    results = pl.pallas_call(
        functools.partial(kernel, rollouts),
        out_shape=tuple(pltpu.VMEM(shape, f32) for shape in shapes),
        in_specs=[any_space] * 6,
        out_specs=(vmem, vmem, vmem),
        scratch_shapes=[
            pltpu.VMEM((TOKENS, D), jnp.bfloat16),
            pltpu.VMEM((NB, D), jnp.bfloat16),
            pltpu.VMEM((1, NB), f32),
            pltpu.VMEM((1, TOKENS), f32),
            pltpu.VMEM((1, TOKENS), jnp.int32),
            pltpu.VMEM((1, TOKENS), jnp.int32),
            pltpu.VMEM((1, TOKENS), f32),
            pltpu.VMEM((NB, TOKENS), jnp.bfloat16),
            pair, pair, single, single,
            pltpu.VMEM((4, NB, 4 * QUARTER), f32),
            pltpu.VMEM((4, 32, 4 * QUARTER), f32),
            pltpu.VMEM((4, 32, 4 * QUARTER), f32),
            pltpu.VMEM((2, 2, 3, 32, QUARTER), f32),
            pltpu.VMEM((2, 2, 32, QUARTER), f32),
            pltpu.VMEM((2, 7, 8, QUARTER), f32),
            pltpu.VMEM((2, 4, 8, QUARTER), f32),
            dma((PIECES,)), dma((5,)), dma((4,)), dma((4,)),
            dma((4,)), dma((4,)), dma((2, 2, 3)), dma((2, 2, 3)), dma((2, 7)), dma((2, 7)), dma((2, 3)), dma((2, 3)),
            dma((2, 7)), dma((2, 7)), dma((2, 3)), dma((2, 3)), dma((2, 4)), dma((2, 4)),
        ],
        compiler_params=pltpu.CompilerParams(
            collective_id=0, has_side_effects=True, vmem_limit_bytes=60 * 1024 * 1024
        ),
    )(hidden, value_weight.T, value_bias.reshape(1, NB), returns, task_bins, loss_mask)
    targets, grad, bias_grad = pl.pallas_call(
        write_out,
        out_shape=tuple(jax.ShapeDtypeStruct(shape, f32) for shape in shapes),
        in_specs=[vmem] * 3,
        out_specs=(any_space,) * 3,
        scratch_shapes=[dma((3,))],
    )(*(pltpu.with_memory_space_constraint(r, pltpu.VMEM) for r in results))
    return targets, grad.T, bias_grad.reshape(NB)


def solution(mesh):
    torus = Mesh(mesh.devices.reshape(NX, NZ, NY, NC), ("x", "z", "y", "c"))
    dp, seq = ("x", "z"), ("y", "c")
    return jax.shard_map(
        on_device,
        mesh=torus,
        in_specs=(P(dp, seq, None), P(), P(), P(dp, seq), P(dp, seq), P(dp, seq)),
        out_specs=(P(dp, seq), P(), P()),
        check_vma=False,
    )
```
